512 devices in a mesh: gx: 16 (over y_lo, x, core), gy: 32 (over y_hi, z).
Axes of the slice: x: 4, y: 8 (y_hi: 4, y_lo: 2; y = y_hi * 2 + y_lo), z: 8, core: 2. Of those that a mesh axis runs over, the one named last changes fastest.
Arguments:
- activation: bfloat16 [32, 64, 128, 128], P(None, 'gx', 'gy'), may hold values from -6 to 6
- out_grad: bfloat16 [32, 64, 128, 128], P(None, 'gx', 'gy'), may hold values from -6 to 6
- kernel: bfloat16 [3, 3, 3, 32, 32], replicated, may hold values from -0.21875 to 0.21875
Outputs:
- grad_input: bfloat16 [32, 64, 128, 128], P(None, 'gx', 'gy')
- grad_kernel: float32 [3, 3, 3, 32, 32], replicated
The draws below stay inside these ranges and needn't reach their ends.
All inputs are finite; a program needn't handle non-finite values.
Results may differ from the reference program's by a relative error of at most 0.001.
Values may be sent and summed in bfloat16 or wider, within the bound.
A program may use at most 64 MiB of HBM per device.

```python
import jax
import jax.numpy as jnp

C = 32
NZ = 128
NX = 64
NY = 128


def shard_levels(stream_key, dims, shards, low, high):
    level = 1.0
    for dim, parts in shards:
        steps = jax.random.uniform(jax.random.fold_in(jax.random.fold_in(stream_key, 6), dim), (parts,), jnp.float32, low / len(shards), high / len(shards))
        level = level * jnp.repeat(jnp.exp(steps), dims[dim] // parts).reshape((-1,) + (1,) * (len(dims) - 1 - dim))
    return level


def bell_draw(stream_key, dims, spread, reach, shards=(), held_as=jnp.bfloat16):
    level = shard_levels(stream_key, dims, shards, -0.22, 0.18) if shards else 1.0
    values = jax.random.normal(stream_key, dims, jnp.float32) * spread * level
    return jnp.minimum(jnp.maximum(values, -reach), reach).astype(held_as)


def setup_inputs(seed: int = 0) -> dict:
    key_list = jax.random.split(jax.random.key(seed), 4)
    return {
        "activation": bell_draw(key_list[0], (C, NX, NY, NZ), 1.0, 6.0, ((1, 16), (2, 32))),
        "out_grad": bell_draw(key_list[1], (C, NX, NY, NZ), 1.0, 6.0, ((1, 16), (2, 32))),
        "kernel": bell_draw(key_list[2], (3, 3, 3, C, C), (27 * C) ** -0.5, 0.21875),
    }


def reference(activation, out_grad, kernel):
    channels = activation.shape[0]
    size_x, size_y, size_z = (activation.shape[1], activation.shape[2], activation.shape[3])
    cell_count = size_x * size_y * size_z
    grad_pad = jnp.pad(out_grad, ((0, 0), (1, 1), (1, 1), (1, 1)))
    act_pad = jnp.pad(activation, ((0, 0), (1, 1), (1, 1), (1, 1)))
    flat_grad = out_grad.reshape(channels, cell_count)
    accumulated = jnp.zeros((channels, cell_count), jnp.float32)
    products = []
    for off_x in range(3):
        for off_y in range(3):
            for off_z in range(3):
                window = grad_pad[:, 2 - off_x:2 - off_x + size_x, 2 - off_y:2 - off_y + size_y, 2 - off_z:2 - off_z + size_z].reshape(channels, cell_count)
                accumulated = accumulated + jnp.dot(kernel[off_x, off_y, off_z].T, window, preferred_element_type=jnp.float32)
                shifted = act_pad[:, off_x:off_x + size_x, off_y:off_y + size_y, off_z:off_z + size_z].reshape(channels, cell_count)
                products.append(jnp.dot(flat_grad, shifted.T, preferred_element_type=jnp.float32))
    grad_input = accumulated.reshape(channels, size_x, size_y, size_z).astype(jnp.bfloat16)
    raw = jnp.stack(products).reshape(3, 3, 3, channels, channels)
    grad_kernel = raw / jnp.sqrt(jnp.float32(NX * NY * NZ))
    return (grad_input, grad_kernel)
```

```python
import functools
import math

import jax
import jax.numpy as jnp
from jax import lax
from jax.experimental import pallas as pl
from jax.experimental.pallas import tpu as pltpu
from jax.sharding import PartitionSpec as P

MESH = pl.DeviceIdType.MESH
F32 = jnp.float32
BF16 = jnp.bfloat16
LOW = 2


def far_first(count):
    return sorted(range(1, count), key=lambda d: -min(d, count - d))


def kernel(
    sizes, scale, act_ref, g_ref, k_ref, gi_ref, gk_ref,
    rows, halo, acts, total, kmat, part, from_a, sum_a, from_y, from_z, final,
    halo_send, halo_recv, a_send, a_recv, y_send, y_recv, z_send, z_recv,
    yg_send, yg_recv, ag_send, ag_recv,
):
    n_gx, n_gy, n_a, n_y, n_z, chans, size_x, size_y, size_z = sizes
    cols = size_x * size_y
    gx = lax.axis_index("gx")
    gy = lax.axis_index("gy")
    a = lax.rem(gx, n_a)
    y = lax.div(gy, n_z) * LOW + lax.div(gx, n_a)
    z = lax.rem(gy, n_z)

    def a_peer(d):
        return (lax.div(gx, n_a) * n_a + lax.rem(a + d, n_a), gy)

    def y_peer(d):
        other = lax.rem(y + d, n_y)
        return (lax.rem(other, LOW) * n_a + a, lax.div(other, LOW) * n_z + z)

    def z_peer(d):
        return (gx, lax.div(gy, n_z) * n_z + lax.rem(z + d, n_z))

    def halo_peer(dx, dy):
        return (lax.rem(gx + dx + n_gx, n_gx), lax.rem(gy + dy + n_gy, n_gy))

    steps = [(dx, dy) for dx in (-1, 0, 1) for dy in (-1, 0, 1) if dx or dy]
    steps.sort(key=lambda s: -abs(s[0]) - 2 * abs(s[1]))
    peers = [halo_peer(*s) for s in steps]
    peers += [a_peer(d) for d in far_first(n_a)]
    peers += [y_peer(d) for d in far_first(n_y)]
    peers += [z_peer(d) for d in far_first(n_z)]
    barrier = pltpu.get_barrier_semaphore()
    for peer in peers:
        pl.semaphore_signal(barrier, inc=1, device_id=peer, device_id_type=MESH)

    rows[...] = g_ref[...].astype(F32)
    for i in range(size_x):
        for j in range(size_y):
            col = rows[pl.ds(i * size_y + j, chans, stride=cols), :]
            halo[i + 1, j + 1] = col.astype(BF16)

    pl.semaphore_wait(barrier, len(peers))

    def span(step, size):
        if step == 0:
            return slice(1, size + 1), slice(1, size + 1)
        return (slice(size, size + 1), slice(0, 1)) if step > 0 else (slice(1, 2), slice(size + 1, size + 2))

    copies = []
    for n, (dx, dy) in enumerate(steps):
        src_x, dst_x = span(dx, size_x)
        src_y, dst_y = span(dy, size_y)
        copy = pltpu.make_async_remote_copy(
            src_ref=halo.at[src_x, src_y],
            dst_ref=halo.at[dst_x, dst_y],
            send_sem=halo_send.at[n],
            recv_sem=halo_recv.at[n],
            device_id=halo_peer(dx, dy),
            device_id_type=MESH,
        )
        copy.start()
        copies.append(copy)

    lane = lax.broadcasted_iota(jnp.int32, (chans, size_z), 1)

    def shifted(tile, step):
        if step == 0:
            return tile
        moved = pltpu.roll(tile, step % size_z, 1)
        edge = 0 if step > 0 else size_z - 1
        return jnp.where(lane == edge, 0.0, moved)

    rows[...] = act_ref[...].astype(F32)
    for i in range(size_x):
        for j in range(size_y):
            col = rows[pl.ds(i * size_y + j, chans, stride=cols), :]
            for c in range(3):
                acts[i, j, pl.ds(c * chans, chans)] = shifted(col, 1 - c).astype(BF16)

    for copy in copies:
        copy.wait_recv()

    def blank(index):
        halo[index] = jnp.zeros(halo.at[index].shape, BF16)

    @pl.when(gx == 0)
    def _():
        blank((slice(0, 1),))

    @pl.when(gx == n_gx - 1)
    def _():
        blank((slice(size_x + 1, size_x + 2),))

    @pl.when(gy == 0)
    def _():
        blank((slice(None), slice(0, 1)))

    @pl.when(gy == n_gy - 1)
    def _():
        blank((slice(None), slice(size_y + 1, size_y + 2)))

    def windows(i):
        columns = []
        for j in range(size_y):
            tiles = [halo[i + 2 - off_x, j + 2 - off_y] for off_x in range(3) for off_y in range(3)]
            columns.append(jnp.concatenate(tiles, axis=0))
        return jnp.concatenate(columns, axis=1)

    total[...] = jnp.zeros_like(total)
    for i in range(size_x):
        right = jnp.concatenate([acts[i, j] for j in range(size_y)], axis=1)
        total[:, 0 : 3 * chans] += lax.dot_general(
            windows(i), right, (((1,), (1,)), ((), ())), preferred_element_type=F32
        )

    piece = part.shape[2]

    def put(row, block):
        for s in range(0, chans, piece):
            at = (row * chans + s) // piece
            part[at // n_y, at % n_y] = block[s : s + piece]

    wide = lax.broadcasted_iota(jnp.int32, (chans, 4 * chans), 1)
    for r in range(8):
        if r == 7:
            put(r, jnp.zeros((chans, 4 * chans), F32))
            continue
        block = total[pl.ds(r * chans, chans), :]
        if r < 6:
            extra = total[pl.ds((7 + r // 3) * chans, chans), :]
            extra = pltpu.roll(extra, (3 - r % 3) * chans, 1)
            block = jnp.where(wide < 3 * chans, block, extra)
        put(r, block)

    def send(src, dst, send_sem, recv_sem, peer):
        copy = pltpu.make_async_remote_copy(
            src_ref=src, dst_ref=dst, send_sem=send_sem, recv_sem=recv_sem,
            device_id=peer, device_id_type=MESH,
        )
        copy.start()
        copies.append(copy)
        return copy

    flying = [
        send(part.at[lax.rem(a + d, n_a)], from_a.at[d], a_send.at[d], a_recv.at[d], a_peer(d))
        for d in far_first(n_a)
    ]

    kmat[...] = jnp.zeros_like(kmat)
    for ab in range(9):
        for c in range(3):
            kmat[pl.ds(ab * chans, chans), pl.ds(c * chans, chans)] = k_ref[
                pl.ds((ab * 3 + c) * chans, chans), :
            ].astype(F32)
    left = kmat[...].T[0 : 3 * chans, 0 : 9 * chans].astype(BF16)
    for i in range(size_x):
        sums = jnp.dot(left, windows(i), preferred_element_type=F32)
        for j in range(size_y):
            tile = sums[:, j * size_z : (j + 1) * size_z]
            value = shifted(tile[0:chans], -1) + tile[chans : 2 * chans] + shifted(tile[2 * chans :], 1)
            rows[pl.ds(i * size_y + j, chans, stride=cols), :] = value
    gi_ref[...] = rows[...].astype(BF16)

    def arrived(flying):
        for copy in flying:
            copy.wait_recv()

    arrived(flying)
    value = part[a]
    for d in range(1, n_a):
        value = value + from_a[d]
    sum_a[...] = value
    flying = [
        send(sum_a.at[lax.rem(y + d, n_y)], from_y.at[d], y_send.at[d], y_recv.at[d], y_peer(d))
        for d in far_first(n_y)
    ]
    arrived(flying)
    value = sum_a[y]
    for d in range(1, n_y):
        value = value + from_y[d]
    from_z[z] = value
    flying = [
        send(from_z.at[z], from_z.at[z], z_send.at[d], z_recv.at[d], z_peer(d))
        for d in far_first(n_z)
    ]
    arrived(flying)
    value = from_z[0]
    for d in range(1, n_z):
        value = value + from_z[d]
    final[a, y] = value * scale
    flying = [
        send(final.at[a, y], final.at[a, y], yg_send.at[d], yg_recv.at[d], y_peer(d))
        for d in far_first(n_y)
    ]
    arrived(flying)
    flying = [
        send(final.at[a], final.at[a], ag_send.at[d], ag_recv.at[d], a_peer(d))
        for d in far_first(n_a)
    ]
    arrived(flying)

    for r in range(7):
        for s in range(0, chans, piece):
            at = (r * chans + s) // piece
            block = final[at // n_y, at % n_y]
            for c in range(4):
                if c < 3:
                    place = r * 3 + c
                elif r < 6:
                    place = 21 + r
                else:
                    continue
                gk_ref[pl.ds(place * chans + s, piece), :] = block[:, c * chans : (c + 1) * chans]

    for copy in copies:
        copy.wait_send()


def solution(mesh):
    n_gx, n_gy = mesh.shape["gx"], mesh.shape["gy"]
    n_a = n_gx // LOW
    n_z = 8 if n_gy % 8 == 0 else 2
    n_y = n_gy // n_z * LOW

    def step(activation, out_grad, weights):
        chans, size_x, size_y, size_z = activation.shape
        cols = size_x * size_y
        cells = n_gx * size_x * n_gy * size_y * size_z
        piece = 8 * chans // (n_a * n_y)
        sizes = (n_gx, n_gy, n_a, n_y, n_z, chans, size_x, size_y, size_z)
        vmem = pl.BlockSpec(memory_space=pltpu.VMEM)
        dma = pltpu.SemaphoreType.DMA
        grad_input, grad_kernel = pl.pallas_call(
            functools.partial(kernel, sizes, 1.0 / math.sqrt(cells)),
            out_shape=(
                jax.ShapeDtypeStruct((chans * cols, size_z), BF16),
                jax.ShapeDtypeStruct((27 * chans, chans), F32),
            ),
            in_specs=[vmem] * 3,
            out_specs=(vmem, vmem),
            scratch_shapes=[
                pltpu.VMEM((chans * cols, size_z), F32),
                pltpu.VMEM((size_x + 2, size_y + 2, chans, size_z), BF16),
                pltpu.VMEM((size_x, size_y, 3 * chans, size_z), BF16),
                pltpu.VMEM((9 * chans, 4 * chans), F32),
                pltpu.VMEM((12 * chans, 4 * chans), F32),
                pltpu.VMEM((n_a, n_y, piece, 4 * chans), F32),
                pltpu.VMEM((n_a, n_y, piece, 4 * chans), F32),
                pltpu.VMEM((n_y, piece, 4 * chans), F32),
                pltpu.VMEM((n_y, piece, 4 * chans), F32),
                pltpu.VMEM((n_z, piece, 4 * chans), F32),
                pltpu.VMEM((n_a, n_y, piece, 4 * chans), F32),
                dma((8,)), dma((8,)),
                dma((n_a,)), dma((n_a,)),
                dma((n_y,)), dma((n_y,)),
                dma((n_z,)), dma((n_z,)),
                dma((n_y,)), dma((n_y,)),
                dma((n_a,)), dma((n_a,)),
            ],
            compiler_params=pltpu.CompilerParams(collective_id=0, has_side_effects=True),
        )(
            activation.reshape(chans * cols, size_z),
            out_grad.reshape(chans * cols, size_z),
            weights.reshape(27 * chans, chans),
        )
        return (
            grad_input.reshape(chans, size_x, size_y, size_z),
            grad_kernel.reshape(3, 3, 3, chans, chans),
        )

    return jax.shard_map(
        step,
        mesh=mesh,
        in_specs=(P(None, "gx", "gy", None), P(None, "gx", "gy", None), P()),
        out_specs=(P(None, "gx", "gy", None), P()),
        check_vma=False,
    )
```

```python
import functools
import math

import jax
import jax.numpy as jnp
from jax import lax
from jax.experimental import pallas as pl
from jax.experimental.pallas import tpu as pltpu
from jax.sharding import PartitionSpec as P

MESH = pl.DeviceIdType.MESH
F32 = jnp.float32
BF16 = jnp.bfloat16
LOW = 2


def far_first(count):
    return sorted(range(1, count), key=lambda d: -min(d, count - d))


def kernel(
    sizes, scale, act_hbm, g_hbm, k_hbm, gi_ref, gk_ref,
    act_ref, g_ref, k_ref, loaded, rows, halo, acts, total, kmat, part, from_a, sum_a, from_y, from_z, final,
    halo_send, halo_recv, a_send, a_recv, y_send, y_recv, z_send, z_recv,
    yg_send, yg_recv, ag_send, ag_recv,
):
    n_gx, n_gy, n_a, n_y, n_z, chans, size_x, size_y, size_z = sizes
    cols = size_x * size_y
    gx = lax.axis_index("gx")
    gy = lax.axis_index("gy")
    a = lax.rem(gx, n_a)
    y = lax.div(gy, n_z) * LOW + lax.div(gx, n_a)
    z = lax.rem(gy, n_z)

    def a_peer(d):
        return (lax.div(gx, n_a) * n_a + lax.rem(a + d, n_a), gy)

    def y_peer(d):
        other = lax.rem(y + d, n_y)
        return (lax.rem(other, LOW) * n_a + a, lax.div(other, LOW) * n_z + z)

    def z_peer(d):
        return (gx, lax.div(gy, n_z) * n_z + lax.rem(z + d, n_z))

    def halo_peer(dx, dy):
        return (lax.rem(gx + dx + n_gx, n_gx), lax.rem(gy + dy + n_gy, n_gy))

    steps = [(dx, dy) for dx in (-1, 0, 1) for dy in (-1, 0, 1) if dx or dy]
    steps.sort(key=lambda s: -abs(s[0]) - 2 * abs(s[1]))
    peers = [halo_peer(*s) for s in steps]
    peers += [a_peer(d) for d in far_first(n_a)]
    peers += [y_peer(d) for d in far_first(n_y)]
    peers += [z_peer(d) for d in far_first(n_z)]
    barrier = pltpu.get_barrier_semaphore()
    for peer in peers:
        pl.semaphore_signal(barrier, inc=1, device_id=peer, device_id_type=MESH)

    loads = [
        pltpu.make_async_copy(src, dst, loaded.at[n])
        for n, (src, dst) in enumerate([(g_hbm, g_ref), (act_hbm, act_ref), (k_hbm, k_ref)])
    ]
    for load in loads:
        load.start()

    loads[0].wait()
    rows[...] = g_ref[...].astype(F32)
    for i in range(size_x):
        for j in range(size_y):
            col = rows[pl.ds(i * size_y + j, chans, stride=cols), :]
            halo[i + 1, j + 1] = col.astype(BF16)

    pl.semaphore_wait(barrier, len(peers))

    def span(step, size):
        if step == 0:
            return slice(1, size + 1), slice(1, size + 1)
        return (slice(size, size + 1), slice(0, 1)) if step > 0 else (slice(1, 2), slice(size + 1, size + 2))

    copies = []
    for n, (dx, dy) in enumerate(steps):
        src_x, dst_x = span(dx, size_x)
        src_y, dst_y = span(dy, size_y)
        copy = pltpu.make_async_remote_copy(
            src_ref=halo.at[src_x, src_y],
            dst_ref=halo.at[dst_x, dst_y],
            send_sem=halo_send.at[n],
            recv_sem=halo_recv.at[n],
            device_id=halo_peer(dx, dy),
            device_id_type=MESH,
        )
        copy.start()
        copies.append(copy)

    lane = lax.broadcasted_iota(jnp.int32, (chans, size_z), 1)

    def shifted(tile, step):
        if step == 0:
            return tile
        moved = pltpu.roll(tile, step % size_z, 1)
        edge = 0 if step > 0 else size_z - 1
        return jnp.where(lane == edge, 0.0, moved)

    loads[1].wait()
    rows[...] = act_ref[...].astype(F32)
    for i in range(size_x):
        for j in range(size_y):
            col = rows[pl.ds(i * size_y + j, chans, stride=cols), :]
            for c in range(3):
                acts[i, j, pl.ds(c * chans, chans)] = shifted(col, 1 - c).astype(BF16)

    for copy in copies:
        copy.wait_recv()

    def blank(index):
        halo[index] = jnp.zeros(halo.at[index].shape, BF16)

    @pl.when(gx == 0)
    def _():
        blank((slice(0, 1),))

    @pl.when(gx == n_gx - 1)
    def _():
        blank((slice(size_x + 1, size_x + 2),))

    @pl.when(gy == 0)
    def _():
        blank((slice(None), slice(0, 1)))

    @pl.when(gy == n_gy - 1)
    def _():
        blank((slice(None), slice(size_y + 1, size_y + 2)))

    def windows(i):
        columns = []
        for j in range(size_y):
            tiles = [halo[i + 2 - off_x, j + 2 - off_y] for off_x in range(3) for off_y in range(3)]
            columns.append(jnp.concatenate(tiles, axis=0))
        return jnp.concatenate(columns, axis=1)

    total[...] = jnp.zeros_like(total)
    for i in range(size_x):
        right = jnp.concatenate([acts[i, j] for j in range(size_y)], axis=1)
        total[:, 0 : 3 * chans] += lax.dot_general(
            windows(i), right, (((1,), (1,)), ((), ())), preferred_element_type=F32
        )

    piece = part.shape[2]

    def put(row, block):
        for s in range(0, chans, piece):
            at = (row * chans + s) // piece
            part[at // n_y, at % n_y] = block[s : s + piece]

    wide = lax.broadcasted_iota(jnp.int32, (chans, 4 * chans), 1)
    for r in range(8):
        if r == 7:
            put(r, jnp.zeros((chans, 4 * chans), F32))
            continue
        block = total[pl.ds(r * chans, chans), :]
        if r < 6:
            extra = total[pl.ds((7 + r // 3) * chans, chans), :]
            extra = pltpu.roll(extra, (3 - r % 3) * chans, 1)
            block = jnp.where(wide < 3 * chans, block, extra)
        put(r, block)

    def send(src, dst, send_sem, recv_sem, peer):
        copy = pltpu.make_async_remote_copy(
            src_ref=src, dst_ref=dst, send_sem=send_sem, recv_sem=recv_sem,
            device_id=peer, device_id_type=MESH,
        )
        copy.start()

    def landed(ref, sem):
        pltpu.make_async_copy(ref, ref, sem).wait()

    for dy in far_first(n_y) + [0]:
        for d in far_first(n_a):
            send(
                part.at[lax.rem(a + d, n_a), lax.rem(y + dy, n_y)], from_a.at[dy, d],
                a_send, a_recv.at[dy], a_peer(d),
            )

    loads[2].wait()
    kmat[...] = jnp.zeros_like(kmat)
    for ab in range(9):
        for c in range(3):
            kmat[pl.ds(ab * chans, chans), pl.ds(c * chans, chans)] = k_ref[
                pl.ds((ab * 3 + c) * chans, chans), :
            ].astype(F32)
    left = kmat[...].T[0 : 3 * chans, 0 : 9 * chans].astype(BF16)
    for i in range(size_x):
        sums = jnp.dot(left, windows(i), preferred_element_type=F32)
        for j in range(size_y):
            tile = sums[:, j * size_z : (j + 1) * size_z]
            value = shifted(tile[0:chans], -1) + tile[chans : 2 * chans] + shifted(tile[2 * chans :], 1)
            rows[pl.ds(i * size_y + j, chans, stride=cols), :] = value
    gi_ref[...] = rows[...].astype(BF16)

    for dy in far_first(n_y) + [0]:
        landed(from_a.at[dy, 1:], a_recv.at[dy])
        value = part[a, lax.rem(y + dy, n_y)]
        for d in range(1, n_a):
            value = value + from_a[dy, d]
        if dy:
            sum_a[dy] = value
            send(sum_a.at[dy], from_y.at[dy], y_send, y_recv, y_peer(dy))
    landed(from_y.at[1:], y_recv)
    for d in range(1, n_y):
        value = value + from_y[d]

    from_z[z] = value
    for d in far_first(n_z):
        send(from_z.at[z], from_z.at[z], z_send, z_recv, z_peer(d))
    landed(from_z.at[1:], z_recv)
    value = from_z[0]
    for d in range(1, n_z):
        value = value + from_z[d]

    final[a, y] = value * scale
    for dy in far_first(n_y):
        send(final.at[a, y], final.at[a, y], yg_send, yg_recv.at[dy], y_peer(dy))
    for dy in [0] + far_first(n_y)[::-1]:
        source = lax.rem(y - dy + n_y, n_y)
        piece_ref = final.at[a, source]
        if dy:
            landed(piece_ref, yg_recv.at[dy])
        for d in far_first(n_a):
            send(piece_ref, piece_ref, ag_send, ag_recv, a_peer(d))
    landed(final.at[1:], ag_recv)

    for r in range(7):
        for s in range(0, chans, piece):
            at = (r * chans + s) // piece
            block = final[at // n_y, at % n_y]
            for c in range(4):
                if c < 3:
                    place = r * 3 + c
                elif r < 6:
                    place = 21 + r
                else:
                    continue
                gk_ref[pl.ds(place * chans + s, piece), :] = block[:, c * chans : (c + 1) * chans]

    for copy in copies:
        copy.wait_send()
    landed(part.at[1:], a_send)
    landed(sum_a.at[1:], y_send)
    landed(from_z.at[1:], z_send)
    landed(sum_a.at[1:], yg_send)
    landed(final.at[1:], ag_send)


def solution(mesh):
    n_gx, n_gy = mesh.shape["gx"], mesh.shape["gy"]
    n_a = n_gx // LOW
    n_z = 8 if n_gy % 8 == 0 else 2
    n_y = n_gy // n_z * LOW

    def step(activation, out_grad, weights):
        chans, size_x, size_y, size_z = activation.shape
        cols = size_x * size_y
        cells = n_gx * size_x * n_gy * size_y * size_z
        piece = 8 * chans // (n_a * n_y)
        sizes = (n_gx, n_gy, n_a, n_y, n_z, chans, size_x, size_y, size_z)
        vmem = pl.BlockSpec(memory_space=pltpu.VMEM)
        dma = pltpu.SemaphoreType.DMA
        grad_input, grad_kernel = pl.pallas_call(
            functools.partial(kernel, sizes, 1.0 / math.sqrt(cells)),
            out_shape=(
                pltpu.VMEM((chans * cols, size_z), BF16),
                pltpu.VMEM((27 * chans, chans), F32),
            ),
            in_specs=[pl.BlockSpec(memory_space=pl.ANY)] * 3,
            out_specs=(vmem, vmem),
            scratch_shapes=[
                pltpu.VMEM((chans * cols, size_z), BF16),
                pltpu.VMEM((chans * cols, size_z), BF16),
                pltpu.VMEM((27 * chans, chans), BF16),
                dma((3,)),
                pltpu.VMEM((chans * cols, size_z), F32),
                pltpu.VMEM((size_x + 2, size_y + 2, chans, size_z), BF16),
                pltpu.VMEM((size_x, size_y, 3 * chans, size_z), BF16),
                pltpu.VMEM((9 * chans, 4 * chans), F32),
                pltpu.VMEM((12 * chans, 4 * chans), F32),
                pltpu.VMEM((n_a, n_y, piece, 4 * chans), F32),
                pltpu.VMEM((n_y, n_a, piece, 4 * chans), F32),
                pltpu.VMEM((n_y, piece, 4 * chans), F32),
                pltpu.VMEM((n_y, piece, 4 * chans), F32),
                pltpu.VMEM((n_z, piece, 4 * chans), F32),
                pltpu.VMEM((n_a, n_y, piece, 4 * chans), F32),
                dma((8,)), dma((8,)),
                dma, dma((n_y,)),
                dma, dma,
                dma, dma,
                dma, dma((n_y,)),
                dma, dma,
            ],
            compiler_params=pltpu.CompilerParams(collective_id=0, has_side_effects=True),
        )(
            activation.reshape(chans * cols, size_z),
            out_grad.reshape(chans * cols, size_z),
            weights.reshape(27 * chans, chans),
        )
        return (
            grad_input.reshape(chans, size_x, size_y, size_z),
            grad_kernel.reshape(3, 3, 3, chans, chans),
        )

    return jax.shard_map(
        step,
        mesh=mesh,
        in_specs=(P(None, "gx", "gy", None), P(None, "gx", "gy", None), P()),
        out_specs=(P(None, "gx", "gy", None), P()),
        check_vma=False,
    )
```
